256 devices in a mesh: blk: 64 (over y, z, x_hi), tp: 4 (over x_lo, core).
Axes of the slice: x: 4 (x_hi: 2, x_lo: 2; x = x_hi * 2 + x_lo), y: 4, z: 8, core: 2. Of those that a mesh axis runs over, the one named last changes fastest.
Arguments:
- kv_keys: bfloat16 [256, 2048, 512], P('blk', None, 'tp'), may hold values from -6 to 6
- kv_values: bfloat16 [256, 2048, 512], P('blk', None, 'tp'), may hold values from -6 to 6
- queries: bfloat16 [256, 128, 3584], P('blk', None, 'tp'), may hold values from -170 to 170, as said below
- hidden: bfloat16 [256, 128, 3584], P('blk', None, 'tp'), may hold values from -2 to 2
- out_weight: bfloat16 [3584, 3584], P('tp'), may hold values from -0.09375 to 0.09375
- block_live: int32 [256], P('blk'), may hold values from 1 to 128
- node_tiles: int32 [256, 128], P('blk'), may hold values from 1 to 16
- left_count: int32 [64], P('blk'), may hold values from 1 to 2, as said below
- right_count: int32 [64], P('blk'), may hold values from 1 to 2, as said below
Outputs:
- balanced: bfloat16 [512, 128, 3584], P('blk', None, 'tp')
The draws below stay inside these ranges and needn't reach their ends.
Inputs may be any that keep to these rules, and one draw needn't show every extreme that they name: `queries`: queries of the nodes. `left_count`: at most 2; some index reaches 2 in every draw. `right_count`: at most 2; some index reaches 2 in every draw.
All inputs are finite; a program needn't handle non-finite values.
Results may differ from the reference program's by a relative error of at most 0.0047.
Values may be sent and summed in bfloat16 or wider, within the bound.
A program may use at most 192 MiB of HBM per device.

```python
import jax
import jax.numpy as jnp
from jax import lax

D = 3584
QH = 28
KVH = 4
HD = 128
BT = 2048
TILE = 128
BLK_DEV = 4
S_MAX = 2
NPB = 128
TILES = 16
SLOTS = 8
BLOCKS = 256
N_BLK = 64


def pair_draw(key):
    base = jax.random.fold_in(key, 101)
    key_part = jnp.clip(jax.random.normal(jax.random.fold_in(base, 1), (BLOCKS, BT, KVH, HD), jnp.float32), -6.0, 6.0)
    query_part = jnp.clip(2.0 * jax.random.normal(jax.random.fold_in(base, 2), (BLOCKS, NPB, QH, HD), jnp.float32), -12.0, 12.0)
    return (key_part.reshape(BLOCKS, BT, KVH * HD), query_part.reshape(BLOCKS, NPB, QH * HD))


def draw_kv_keys(key, part):
    return pair_draw(key)[0].astype(jnp.bfloat16)


def draw_queries(key, part):
    return pair_draw(key)[1].astype(jnp.bfloat16)


def shift_draw(key):
    cycle_size = BLOCKS // BLK_DEV
    drawn = jax.random.randint(jax.random.fold_in(key, 1), (cycle_size,), 1, S_MAX + 1)
    chosen = jax.random.randint(jax.random.fold_in(key, 2), (), 0, cycle_size)
    return jnp.where(jnp.arange(cycle_size) == chosen, S_MAX, drawn).astype(jnp.int32)


def draw_left_count(key, part):
    return shift_draw(jax.random.fold_in(key, 201))


def draw_right_count(key, part):
    return shift_draw(jax.random.fold_in(key, 202))


def place_ends(values, key, low, top_value):
    extent = values.shape
    index_at = [jax.random.randint(jax.random.fold_in(key, axis), (), 0, extent[axis]) for axis in range(len(extent))]
    values = values.at[tuple(index_at)].set(low)
    longest = extent.index(max(extent))
    index_at[longest] = (index_at[longest] + 1) % extent[longest]
    return values.at[tuple(index_at)].set(top_value)


def block_levels(stream_key, shape, shards, smallest, top_value):
    def one(axis_at, blocks):
        draws = jax.random.uniform(jax.random.fold_in(jax.random.fold_in(stream_key, 6), axis_at), (blocks,), jnp.float32, smallest / len(shards), top_value / len(shards))
        return jnp.repeat(jnp.exp(draws), shape[axis_at] // blocks).reshape((-1,) + (1,) * (len(shape) - axis_at - 1))

    loudness = one(*shards[0])
    for cut in shards[1:]:
        loudness = loudness * one(*cut)
    return loudness


def centred(stream_key, shape, deviation, most, shards=(), kind=jnp.bfloat16):
    entries = jax.random.normal(stream_key, shape, jnp.float32) * deviation
    if len(shards) > 0:
        entries = block_levels(stream_key, shape, shards, -0.22, 0.18) * entries
    return jnp.clip(entries, min=-most, max=most).astype(kind)


def setup_inputs(seed: int = 0) -> dict:
    keys = jax.random.split(jax.random.key(seed), 10)
    return {
        "kv_keys": draw_kv_keys(jax.random.fold_in(keys[9], 71), 0),
        "kv_values": centred(keys[1], (BLOCKS, BT, KVH * HD), 1.0, 6.0, ((0, 64), (2, 4))),
        "queries": draw_queries(jax.random.fold_in(keys[9], 71), 0),
        "hidden": centred(keys[3], (BLOCKS, NPB, D), 0.3, 2.0, ((0, 64), (2, 4))),
        "out_weight": centred(keys[4], (QH * HD, D), (QH * HD) ** -0.5, 0.09375, ((0, 4),)),
        "block_live": place_ends(jax.random.randint(keys[5], (BLOCKS,), 1, NPB + 1), jax.random.fold_in(keys[5], 1), 1, NPB).astype(jnp.int32),
        "node_tiles": place_ends(jax.random.randint(keys[6], (BLOCKS, NPB), 1, TILES + 1), jax.random.fold_in(keys[6], 1), 1, TILES).astype(jnp.int32),
        "left_count": draw_left_count(jax.random.fold_in(keys[9], 71), 0),
        "right_count": draw_right_count(jax.random.fold_in(keys[9], 71), 0),
    }


def attend(query_rows, key_rows, value_rows, tiles):
    batch_size, node_count, row_width = query_rows.shape
    head_size = key_rows.shape[2]
    group_size = row_width // head_size
    flat_rows = query_rows.reshape(batch_size, node_count * group_size, head_size).astype(jnp.float32)
    scores = jnp.einsum('srd,spd->srp', flat_rows, key_rows.astype(jnp.float32)) * (head_size ** -0.5)
    reach = jnp.repeat(tiles, group_size, axis=1) * TILE
    places = lax.broadcasted_iota(jnp.int32, (1, 1, key_rows.shape[1]), 2)
    inside = places < reach[:, :, None]
    scores = jnp.where(inside, scores, jnp.float32(-1e30))
    row_max = jnp.max(scores, axis=-1, keepdims=True)
    weights_exp = jnp.where(inside, jnp.exp(scores - row_max), jnp.float32(0.0))
    weights = (weights_exp / jnp.sum(weights_exp, axis=-1, keepdims=True)).astype(jnp.bfloat16)
    mixed = jnp.einsum('srp,spd->srd', weights.astype(jnp.float32), value_rows.astype(jnp.float32))
    return mixed.astype(jnp.bfloat16).reshape(batch_size, node_count, row_width)


def reference(kv_keys, kv_values, queries, hidden, out_weight, block_live, node_tiles, left_count, right_count):
    group_size = QH // KVH

    def one_block(block_items):
        key_block, value_block, query_block, tile_block = block_items
        key_heads = key_block.reshape(BT, KVH, HD).transpose(1, 0, 2)
        value_heads = value_block.reshape(BT, KVH, HD).transpose(1, 0, 2)
        query_heads = query_block.reshape(NPB, KVH, group_size * HD).transpose(1, 0, 2)
        tile_heads = jnp.broadcast_to(tile_block[None, :], (KVH, NPB))
        result = attend(query_heads, key_heads, value_heads, tile_heads)
        return result.transpose(1, 0, 2).reshape(NPB, QH * HD)

    attn = lax.map(one_block, (kv_keys, kv_values, queries, node_tiles))
    projected = jnp.dot(attn.reshape(BLOCKS * NPB, QH * HD), out_weight, preferred_element_type=jnp.float32)
    node_out = hidden.astype(jnp.float32) + projected.reshape(BLOCKS, NPB, D)
    node_live = jnp.arange(NPB, dtype=jnp.int32)[None, :] < block_live[:, None]
    node_out = jnp.where(node_live[:, :, None], node_out, jnp.float32(0.0))
    device = jnp.arange(N_BLK, dtype=jnp.int32)[:, None]
    slot_index = jnp.arange(SLOTS, dtype=jnp.int32)[None, :]
    previous = (device - 1) % N_BLK
    following = (device + 1) % N_BLK
    from_prev = slot_index < S_MAX
    from_next = slot_index >= S_MAX + BLK_DEV
    source_dev = jnp.where(from_prev, previous, jnp.where(from_next, following, device))
    source_blk = jnp.where(from_prev, BLK_DEV - S_MAX + slot_index, jnp.where(from_next, slot_index - S_MAX - BLK_DEV, slot_index - S_MAX))
    own_usable = (source_blk >= left_count[device]) & (source_blk < BLK_DEV - right_count[device])
    usable = jnp.where(from_prev, S_MAX - slot_index <= right_count[previous], jnp.where(from_next, source_blk < left_count[following], own_usable))
    source_index = (source_dev * BLK_DEV + source_blk).reshape(-1).astype(jnp.int32)
    gathered = node_out[source_index]
    return jnp.where(usable.reshape(-1)[:, None, None], gathered, jnp.float32(0.0)).astype(jnp.bfloat16)
```

```python
import functools
import math

import jax
import jax.numpy as jnp
from jax import lax
from jax.experimental import pallas as pl
from jax.experimental.pallas import tpu as pltpu
from jax.sharding import PartitionSpec as P

TILE = 128
HEAD = 128
S_MAX = 2
MASKED = -(2.0**100)
MESH = pl.DeviceIdType.MESH
ORDER = (0, 3, 1, 2)
GROUPS = ((0, 2), (2, 4), (4, 6), (6, 7))
PIECES = ((0, 512), (512, 896))
CHUNK = 512


def block_kernel(
    live_ref, left_ref, right_ref, tiles_ref, k_hbm, v_hbm, q_hbm, hid_hbm, w_hbm,
    out_ref,
    kb, vb, qb, hb, wb, ind, ones, far, sc, pr, ab, keep, snd, rcv, cut,
    k_sem, v_sem, q_sem, h_sem, w_sem, ws_sem, wr_sem, as_sem, ar_sem,
    is_sem, ir_sem, cs_sem, cr_sem,
    *, ring,
):
    blocks, tokens, _ = kb.shape
    nodes, width = qb.shape[1:]
    b = lax.axis_index("blk")
    t = lax.axis_index("tp")
    half = t // 2
    core = t % 2
    prev = (b + ring - 1) % ring
    following = (b + 1) % ring
    partner = (b, 2 * half + 1 - core)
    across = 2 * (1 - half) + core
    peer = (b, across)

    barrier = pltpu.get_barrier_semaphore()
    for other in (partner, peer, (prev, across), (following, across)):
        pl.semaphore_signal(barrier, inc=1, device_id=other, device_id_type=MESH)

    def local(src, dst, sem):
        return pltpu.make_async_copy(src, dst, sem)

    def remote(src, dst, send, recv, device):
        return pltpu.make_async_remote_copy(
            src_ref=src, dst_ref=dst, send_sem=send, recv_sem=recv,
            device_id=device, device_id_type=MESH,
        )

    def columns(quarter):
        return pl.ds(pl.multiple_of(quarter * width, width), width)

    def load_block(j):
        return (
            local(q_hbm.at[j], qb.at[j], q_sem.at[j]),
            local(k_hbm.at[j], kb.at[j], k_sem.at[j]),
            local(v_hbm.at[j], vb.at[j], v_sem.at[j]),
        )

    near_w = [
        local(w_hbm.at[:, columns(2 * h + core)], wb.at[h, pl.ds(0, width)], w_sem.at[n])
        for n, h in enumerate((half, 1 - half))
    ]
    far_w = [
        remote(
            w_hbm.at[:, columns(2 * h + 1 - core)], wb.at[h, pl.ds(width, width)],
            ws_sem.at[n], wr_sem.at[n], partner,
        )
        for n, h in enumerate((half, 1 - half))
    ]
    hid_copy = local(hid_hbm, hb, h_sem)

    for copy in load_block(ORDER[0]):
        copy.start()

    token = lax.broadcasted_iota(jnp.int32, (tokens, HEAD), 0)
    lane = lax.broadcasted_iota(jnp.int32, (tokens, HEAD), 1)
    ind[...] = jnp.where(token // TILE == lane, 1.0, 0.0).astype(jnp.bfloat16)
    ones[...] = jnp.ones_like(ones)
    node_lane = lax.broadcasted_iota(jnp.int32, (nodes, HEAD), 1).astype(jnp.float32)
    for j in range(blocks):
        row = tiles_ref[pl.ds(j, 1), :].astype(jnp.float32)
        reach = jnp.transpose(jnp.broadcast_to(row, (HEAD, nodes)))
        far[j] = jnp.where(node_lane < reach, 0.0, MASKED).astype(jnp.bfloat16)
    zero_rows = jnp.zeros((nodes, width), jnp.bfloat16)
    out_ref[S_MAX] = zero_rows
    out_ref[S_MAX + blocks - 1] = zero_rows

    pl.semaphore_wait(barrier, 4)
    far_w[0].start()
    near_w[0].start()
    for j in ORDER[1:2]:
        for copy in load_block(j):
            copy.start()
    far_w[1].start()
    near_w[1].start()
    hid_copy.start()
    for j in ORDER[2:]:
        for copy in load_block(j):
            copy.start()

    scale = jnp.float32(HEAD**-0.5 * math.log2(math.e))
    attn_copies = {
        j: remote(
            ab.at[j, :, pl.ds(0, width)], ab.at[j, :, pl.ds(width, width)],
            as_sem.at[j], ar_sem.at[j], partner,
        )
        for j in range(blocks)
    }
    inner = {
        (j, n): remote(
            snd.at[j, :, pl.ds(lo, hi - lo)], rcv.at[j, :, pl.ds(lo, hi - lo)],
            is_sem.at[j, n], ir_sem.at[j, n], peer,
        )
        for j in range(blocks)
        for n, (lo, hi) in enumerate(PIECES)
    }
    outer = {
        (j, n): remote(
            cut.at[j, :, pl.ds(lo, hi - lo)],
            out_ref.at[(j + S_MAX + blocks) % (2 * blocks), :, pl.ds(lo, hi - lo)]
            if j < S_MAX
            else out_ref.at[j - S_MAX, :, pl.ds(lo, hi - lo)],
            cs_sem.at[j, n], cr_sem.at[j, n],
            (prev if j < S_MAX else following, across),
        )
        for j in range(blocks)
        for n, (lo, hi) in enumerate(PIECES)
    }
    moved = [
        jnp.int32(1),
        (left_ref[0] >= 2).astype(jnp.int32),
        (right_ref[0] >= 2).astype(jnp.int32),
        jnp.int32(1),
    ]

    def scores(j, g, slot):
        lo, hi = GROUPS[g]
        rows = (hi - lo) * nodes
        q_rows = jnp.concatenate(
            [qb[j, :, h * HEAD : (h + 1) * HEAD] for h in range(lo, hi)], axis=0
        )
        far_rows = jnp.concatenate([far[j]] * (hi - lo), axis=0)
        lhs = jnp.concatenate([q_rows, far_rows], axis=1)
        top = jnp.full((rows, HEAD), -jnp.inf, jnp.float32)
        for c in range(0, tokens, CHUNK):
            rhs = jnp.concatenate([kb[j, c : c + CHUNK, :], ind[c : c + CHUNK, :]], axis=1)
            part = lax.dot_general(
                lhs, rhs, (((1,), (1,)), ((), ())), preferred_element_type=jnp.float32
            )
            sc[slot, :rows, c : c + CHUNK] = part
            for w in range(0, CHUNK, HEAD):
                top = jnp.maximum(top, part[:, w : w + HEAD])
        return jnp.max(top, axis=1, keepdims=True)

    def mix(j, g, slot, top):
        lo, hi = GROUPS[g]
        rows = (hi - lo) * nodes
        total = None
        for c in range(0, tokens, CHUNK):
            part = jnp.exp2((sc[slot, :rows, c : c + CHUNK] - top) * scale).astype(jnp.bfloat16)
            rhs = jnp.concatenate([vb[j, c : c + CHUNK, :], ones[c : c + CHUNK, :]], axis=1)
            term = jnp.dot(part, rhs, preferred_element_type=jnp.float32)
            total = term if total is None else total + term
        mean = (total[:, :HEAD] / total[:, HEAD:]).astype(jnp.bfloat16)
        for n, h in enumerate(range(lo, hi)):
            ab[j, :, h * HEAD : (h + 1) * HEAD] = mean[n * nodes : (n + 1) * nodes]

    def attend(j):
        for copy in load_block(j):
            copy.wait()
        top = scores(j, 0, 0)
        for g in range(len(GROUPS)):
            ahead = scores(j, g + 1, (g + 1) % 2) if g + 1 < len(GROUPS) else None
            mix(j, g, g % 2, top)
            top = ahead

    def project(j):
        h_send = half * moved[j] + (1 - half) * (1 - moved[j])
        rows = ab[j]
        keeps = moved[j] == 0
        for n, (lo, hi) in enumerate(PIECES):
            part = jnp.dot(rows, wb[h_send, :, lo:hi], preferred_element_type=jnp.float32)
            residual = jnp.where(keeps, 0.0, hb[j, :, lo:hi].astype(jnp.float32))
            snd[j, :, lo:hi] = (part + residual).astype(jnp.bfloat16)
            inner[j, n].start()
        for n, (lo, hi) in enumerate(PIECES):
            part = jnp.dot(rows, wb[1 - h_send, :, lo:hi], preferred_element_type=jnp.float32)
            residual = jnp.where(keeps, hb[j, :, lo:hi].astype(jnp.float32), 0.0)
            keep[j, :, lo:hi] = part + residual

    def settle(j):
        for n, (lo, hi) in enumerate(PIECES):
            inner[j, n].wait_recv()
            total = keep[j, :, lo:hi] + rcv[j, :, lo:hi].astype(jnp.float32)
            node = lax.broadcasted_iota(jnp.int32, total.shape, 0)
            cut[j, :, lo:hi] = jnp.where(
                node < live_ref[j] * moved[j], total, 0.0
            ).astype(jnp.bfloat16)
            outer[j, n].start()
            if 0 < j < blocks - 1:
                out_ref[S_MAX + j, :, lo:hi] = jnp.where(
                    node < live_ref[j] * (1 - moved[j]), total, 0.0
                ).astype(jnp.bfloat16)

    def exchange(j, first):
        attn_copies[j].start()
        attn_copies[j].wait()
        if first:
            for copy in far_w + near_w:
                copy.wait()
            hid_copy.wait()

    for n, j in enumerate(ORDER):
        attend(j)
        exchange(j, n == 0)
        project(j)
        if n >= 2:
            settle(ORDER[n - 2])
    for j in ORDER[blocks - 2 :]:
        settle(j)
    for j in range(blocks):
        for n in range(len(PIECES)):
            inner[j, n].wait_send()
            outer[j, n].wait()


def on_device(kv_keys, kv_values, queries, hidden, out_weight, block_live, node_tiles, left_count, right_count, *, ring):
    blocks, tokens, _ = kv_keys.shape
    nodes, width = queries.shape[1:]
    hbm = pl.BlockSpec(memory_space=pltpu.MemorySpace.HBM)
    smem = pl.BlockSpec(memory_space=pltpu.MemorySpace.SMEM)
    vmem = pl.BlockSpec(memory_space=pltpu.MemorySpace.VMEM)
    rows = max(hi - lo for lo, hi in GROUPS) * nodes
    bf16, f32 = jnp.bfloat16, jnp.float32
    dma = pltpu.SemaphoreType.DMA
    pieces = len(PIECES)
    return pl.pallas_call(
        functools.partial(block_kernel, ring=ring),
        out_shape=jax.ShapeDtypeStruct((blocks + 2 * S_MAX, nodes, width), bf16),
        in_specs=[smem, smem, smem, vmem, hbm, hbm, hbm, hbm, hbm],
        out_specs=vmem,
        scratch_shapes=[
            pltpu.VMEM((blocks, tokens, HEAD), bf16),
            pltpu.VMEM((blocks, tokens, HEAD), bf16),
            pltpu.VMEM((blocks, nodes, width), bf16),
            pltpu.VMEM((blocks, nodes, width), bf16),
            pltpu.VMEM((2, 2 * width, width), bf16),
            pltpu.VMEM((tokens, HEAD), bf16),
            pltpu.VMEM((tokens, HEAD), bf16),
            pltpu.VMEM((blocks, nodes, HEAD), bf16),
            pltpu.VMEM((2, rows, tokens), f32),
            pltpu.VMEM((8, 128), bf16),
            pltpu.VMEM((blocks, nodes, 2 * width), bf16),
            pltpu.VMEM((blocks, nodes, width), f32),
            pltpu.VMEM((blocks, nodes, width), bf16),
            pltpu.VMEM((blocks, nodes, width), bf16),
            pltpu.VMEM((blocks, nodes, width), bf16),
            dma((blocks,)), dma((blocks,)), dma((blocks,)), dma, dma((2,)),
            dma((2,)), dma((2,)), dma((blocks,)), dma((blocks,)),
            dma((blocks, pieces)), dma((blocks, pieces)),
            dma((blocks, pieces)), dma((blocks, pieces)),
        ],
        compiler_params=pltpu.CompilerParams(
            collective_id=0, has_side_effects=True, vmem_limit_bytes=56 * 2**20
        ),
        name="rebalanced_attention",
    )(block_live, left_count, right_count, node_tiles, kv_keys, kv_values, queries, hidden, out_weight)


def solution(mesh):
    return jax.shard_map(
        functools.partial(on_device, ring=mesh.shape["blk"]),
        mesh=mesh,
        in_specs=(
            P("blk", None, "tp"),
            P("blk", None, "tp"),
            P("blk", None, "tp"),
            P("blk", None, "tp"),
            P("tp", None),
            P("blk"),
            P("blk", None),
            P("blk"),
            P("blk"),
        ),
        out_specs=P("blk", None, "tp"),
        check_vma=False,
    )
```

```python
import functools
import math

import jax
import jax.numpy as jnp
from jax import lax
from jax.experimental import pallas as pl
from jax.experimental.pallas import tpu as pltpu
from jax.sharding import PartitionSpec as P

TILE = 128
HEAD = 128
S_MAX = 2
MASKED = -(2.0**100)
MESH = pl.DeviceIdType.MESH
ORDER = (0, 3, 1, 2)
GROUPS = ((0, 2), (2, 4), (4, 6), (6, 7))
PIECES = ((0, 256), (256, 512), (512, 896))
LAST_PIECES = ((0, 256), (256, 512), (512, 768), (768, 896))
CHUNK = 512


def pieces_of(j):
    return LAST_PIECES if j == ORDER[-1] else PIECES


def block_kernel(
    live_hbm, left_hbm, right_hbm, tiles_hbm, k_hbm, v_hbm, q_hbm, hid_hbm, w_hbm,
    out_ref,
    live_ref, left_ref, right_ref, tiles_ref,
    kb, vb, qb, hb, wb, ind, ones, far, sc, ab, keep, snd, rcv, cut,
    s_sem, k_sem, v_sem, q_sem, h_sem, w_sem, ws_sem, wr_sem, as_sem, ar_sem,
    is_sem, ir_sem, cs_sem, cr_sem,
    *, ring,
):
    blocks, tokens, _ = kb.shape
    nodes, width = qb.shape[1:]
    b = lax.axis_index("blk")
    t = lax.axis_index("tp")
    half = t // 2
    core = t % 2
    prev = (b + ring - 1) % ring
    following = (b + 1) % ring
    partner = (b, 2 * half + 1 - core)
    across = 2 * (1 - half) + core
    peer = (b, across)

    barrier = pltpu.get_barrier_semaphore()
    for other in (partner, peer, (prev, across), (following, across)):
        pl.semaphore_signal(barrier, inc=1, device_id=other, device_id_type=MESH)

    def local(src, dst, sem):
        return pltpu.make_async_copy(src, dst, sem)

    def remote(src, dst, send, recv, device):
        return pltpu.make_async_remote_copy(
            src_ref=src, dst_ref=dst, send_sem=send, recv_sem=recv,
            device_id=device, device_id_type=MESH,
        )

    q_copies = [local(q_hbm.at[j], qb.at[j], q_sem.at[j]) for j in range(blocks)]
    k_copies = [local(k_hbm.at[j], kb.at[j], k_sem.at[j]) for j in range(blocks)]
    v_copies = [local(v_hbm.at[j], vb.at[j], v_sem.at[j]) for j in range(blocks)]
    small = [
        local(tiles_hbm, tiles_ref, s_sem.at[0]),
        local(live_hbm, live_ref, s_sem.at[1]),
        local(left_hbm, left_ref, s_sem.at[2]),
        local(right_hbm, right_ref, s_sem.at[3]),
    ]
    hid_copy = local(hid_hbm, hb, h_sem)

    weight_parts = [(half, lo, hi) for lo, hi in PIECES] + [(1 - half, 0, width)]

    def weight_from(quarter, lo, hi):
        return w_hbm.at[:, pl.ds(pl.multiple_of(quarter * width + lo, HEAD), hi - lo)]

    near_w = [
        local(
            weight_from(2 * h + core, lo, hi),
            wb.at[h, pl.ds(0, width), pl.ds(lo, hi - lo)], w_sem.at[n],
        )
        for n, (h, lo, hi) in enumerate(weight_parts)
    ]
    far_w = [
        remote(
            weight_from(2 * h + 1 - core, lo, hi),
            wb.at[h, pl.ds(width, width), pl.ds(lo, hi - lo)],
            ws_sem.at[n], wr_sem.at[n], partner,
        )
        for n, (h, lo, hi) in enumerate(weight_parts)
    ]

    for copy in small[:1] + [q_copies[ORDER[0]], k_copies[ORDER[0]], v_copies[ORDER[0]]] + small[1:]:
        copy.start()
    for copy in near_w[:-1]:
        copy.start()
    q_copies[ORDER[1]].start()
    k_copies[ORDER[1]].start()
    v_copies[ORDER[1]].start()

    token = lax.broadcasted_iota(jnp.int32, (tokens, HEAD), 0)
    lane = lax.broadcasted_iota(jnp.int32, (tokens, HEAD), 1)
    ind[...] = jnp.where(token // TILE == lane, 1.0, 0.0).astype(jnp.bfloat16)
    ones[...] = jnp.ones_like(ones)
    zero_rows = jnp.zeros((nodes, width), jnp.bfloat16)
    out_ref[S_MAX] = zero_rows
    out_ref[S_MAX + blocks - 1] = zero_rows
    small[0].wait()
    node_lane = lax.broadcasted_iota(jnp.int32, (nodes, HEAD), 1).astype(jnp.float32)
    for j in range(blocks):
        row = tiles_ref[pl.ds(j, 1), :].astype(jnp.float32)
        reach = jnp.transpose(jnp.broadcast_to(row, (HEAD, nodes)))
        far[j] = jnp.where(node_lane < reach, 0.0, MASKED).astype(jnp.bfloat16)

    def enter():
        pl.semaphore_wait(barrier, 4)
        for copy in far_w[:-1]:
            copy.start()

    scale = jnp.float32(HEAD**-0.5 * math.log2(math.e))
    attn_copies = [
        remote(
            ab.at[j, :, pl.ds(0, width)], ab.at[j, :, pl.ds(width, width)],
            as_sem.at[j], ar_sem.at[j], partner,
        )
        for j in range(blocks)
    ]
    inner = {
        (j, n): remote(
            snd.at[j, :, pl.ds(lo, hi - lo)], rcv.at[j, :, pl.ds(lo, hi - lo)],
            is_sem.at[j, n], ir_sem.at[j, n], peer,
        )
        for j in range(blocks)
        for n, (lo, hi) in enumerate(pieces_of(j))
    }
    outer = {
        (j, n): remote(
            cut.at[j, :, pl.ds(lo, hi - lo)],
            out_ref.at[j + S_MAX + blocks if j < S_MAX else j - S_MAX, :, pl.ds(lo, hi - lo)],
            cs_sem.at[j, n], cr_sem.at[j, n],
            (prev if j < S_MAX else following, across),
        )
        for j in range(blocks)
        for n, (lo, hi) in enumerate(pieces_of(j))
    }

    def moved(j):
        if j == 1:
            return (left_ref[0] >= 2).astype(jnp.int32)
        if j == 2:
            return (right_ref[0] >= 2).astype(jnp.int32)
        return None

    def scores(j, g, slot):
        lo, hi = GROUPS[g]
        rows = (hi - lo) * nodes
        if g == 0:
            q_copies[j].wait()
            k_copies[j].wait()
        q_rows = jnp.concatenate(
            [qb[j, :, h * HEAD : (h + 1) * HEAD] for h in range(lo, hi)], axis=0
        )
        far_rows = jnp.concatenate([far[j]] * (hi - lo), axis=0)
        lhs = jnp.concatenate([q_rows, far_rows], axis=1)
        top = jnp.full((rows, HEAD), -jnp.inf, jnp.float32)
        for c in range(0, tokens, CHUNK):
            rhs = jnp.concatenate([kb[j, c : c + CHUNK, :], ind[c : c + CHUNK, :]], axis=1)
            part = lax.dot_general(
                lhs, rhs, (((1,), (1,)), ((), ())), preferred_element_type=jnp.float32
            )
            sc[slot, :rows, c : c + CHUNK] = part
            for w in range(0, CHUNK, HEAD):
                top = jnp.maximum(top, part[:, w : w + HEAD])
        return jnp.max(top, axis=1, keepdims=True)

    def mix(j, g, slot, top):
        lo, hi = GROUPS[g]
        rows = (hi - lo) * nodes
        if g == 0:
            v_copies[j].wait()
        total = None
        for c in range(0, tokens, CHUNK):
            part = jnp.exp2((sc[slot, :rows, c : c + CHUNK] - top) * scale).astype(jnp.bfloat16)
            rhs = jnp.concatenate([vb[j, c : c + CHUNK, :], ones[c : c + CHUNK, :]], axis=1)
            term = jnp.dot(part, rhs, preferred_element_type=jnp.float32)
            total = term if total is None else total + term
        mean = (total[:, :HEAD] / total[:, HEAD:]).astype(jnp.bfloat16)
        for n, h in enumerate(range(lo, hi)):
            ab[j, :, h * HEAD : (h + 1) * HEAD] = mean[n * nodes : (n + 1) * nodes]

    def residual(j, lo, hi, flag):
        rows = hb[j, :, lo:hi].astype(jnp.float32)
        return rows if flag is None else jnp.where(flag, rows, 0.0)

    def send_part(n):
        j = ORDER[n]
        attn_copies[j].wait()
        move = moved(j)
        pick = half if move is None else half * move + (1 - half) * (1 - move)
        for p, (lo, hi) in enumerate(pieces_of(j)):
            if n == 0:
                near_w[p].wait()
                far_w[p].wait()
            part = jnp.dot(ab[j], wb[pick, :, lo:hi], preferred_element_type=jnp.float32)
            if n == 0 and p == 0:
                hid_copy.wait()
            part = part + residual(j, lo, hi, None if move is None else move == 1)
            snd[j, :, lo:hi] = part.astype(jnp.bfloat16)
            inner[j, p].start()

    def keep_part(n):
        j = ORDER[n]
        move = moved(j)
        if n == 0:
            near_w[-1].wait()
            far_w[-1].wait()
        pick = 1 - half if move is None else half * (1 - move) + (1 - half) * move
        for lo, hi in pieces_of(j):
            part = jnp.dot(ab[j], wb[pick, :, lo:hi], preferred_element_type=jnp.float32)
            if move is not None:
                part = part + residual(j, lo, hi, move == 0)
            keep[j, :, lo:hi] = part

    def settle(n, p):
        j = ORDER[n]
        lo, hi = pieces_of(j)[p]
        move = moved(j)
        inner[j, p].wait_recv()
        total = keep[j, :, lo:hi] + rcv[j, :, lo:hi].astype(jnp.float32)
        node = lax.broadcasted_iota(jnp.int32, total.shape, 0)
        live = live_ref[j]
        leaving = live if move is None else live * move
        cut[j, :, lo:hi] = jnp.where(node < leaving, total, 0.0).astype(jnp.bfloat16)
        outer[j, p].start()
        if move is not None:
            out_ref[S_MAX + j, :, lo:hi] = jnp.where(
                node < live * (1 - move), total, 0.0
            ).astype(jnp.bfloat16)

    def pass_on(n):
        attn_copies[ORDER[n]].start()
        if n == 0:
            far_w[-1].start()

    groups = len(GROUPS)
    units = [(j, g) for j in ORDER for g in range(groups)]
    plan = {
        0: [(enter,)],
        3: [(pass_on, 0)],
        4: [(send_part, 0)],
        7: [(pass_on, 1), (keep_part, 0), (settle, 0, 0)],
        8: [(settle, 0, 1), (send_part, 1)],
        9: [(keep_part, 1), (settle, 0, 2)],
        11: [(pass_on, 2), (settle, 1, 0)],
        12: [(settle, 1, 1), (send_part, 2)],
        13: [(keep_part, 2), (settle, 1, 2)],
        15: [(pass_on, 3), (settle, 2, 0), (send_part, 3), (settle, 2, 1), (keep_part, 3),
             (settle, 2, 2)] + [(settle, 3, p) for p in range(len(LAST_PIECES))],
    }
    for copy in small[1:]:
        copy.wait()
    top = scores(*units[0], 0)
    hid_copy.start()
    near_w[-1].start()
    for j in ORDER[2:]:
        q_copies[j].start()
        k_copies[j].start()
        v_copies[j].start()
    for u, (j, g) in enumerate(units):
        ahead = scores(*units[u + 1], (u + 1) % 2) if u + 1 < len(units) else None
        mix(j, g, u % 2, top)
        top = ahead
        for step, *rest in plan.get(u, ()):
            step(*rest)
    for j in range(blocks):
        for n in range(len(pieces_of(j))):
            inner[j, n].wait_send()
            outer[j, n].wait()


def on_device(kv_keys, kv_values, queries, hidden, out_weight, block_live, node_tiles, left_count, right_count, *, ring):
    blocks, tokens, _ = kv_keys.shape
    nodes, width = queries.shape[1:]
    hbm = pl.BlockSpec(memory_space=pltpu.MemorySpace.HBM)
    vmem = pl.BlockSpec(memory_space=pltpu.MemorySpace.VMEM)
    rows = max(hi - lo for lo, hi in GROUPS) * nodes
    bf16, f32 = jnp.bfloat16, jnp.float32
    dma = pltpu.SemaphoreType.DMA
    pieces = max(len(PIECES), len(LAST_PIECES))
    parts = len(PIECES) + 1
    return pl.pallas_call(
        functools.partial(block_kernel, ring=ring),
        out_shape=pltpu.VMEM((blocks + 2 * S_MAX, nodes, width), bf16),
        in_specs=[hbm] * 9,
        out_specs=vmem,
        scratch_shapes=[
            pltpu.SMEM(block_live.shape, jnp.int32),
            pltpu.SMEM(left_count.shape, jnp.int32),
            pltpu.SMEM(right_count.shape, jnp.int32),
            pltpu.VMEM(node_tiles.shape, jnp.int32),
            pltpu.VMEM((blocks, tokens, HEAD), bf16),
            pltpu.VMEM((blocks, tokens, HEAD), bf16),
            pltpu.VMEM((blocks, nodes, width), bf16),
            pltpu.VMEM((blocks, nodes, width), bf16),
            pltpu.VMEM((2, 2 * width, width), bf16),
            pltpu.VMEM((tokens, HEAD), bf16),
            pltpu.VMEM((tokens, HEAD), bf16),
            pltpu.VMEM((blocks, nodes, HEAD), bf16),
            pltpu.VMEM((2, rows, tokens), f32),
            pltpu.VMEM((blocks, nodes, 2 * width), bf16),
            pltpu.VMEM((blocks, nodes, width), f32),
            pltpu.VMEM((blocks, nodes, width), bf16),
            pltpu.VMEM((blocks, nodes, width), bf16),
            pltpu.VMEM((blocks, nodes, width), bf16),
            dma((4,)), dma((blocks,)), dma((blocks,)), dma((blocks,)), dma, dma((parts,)),
            dma((parts,)), dma((parts,)), dma((blocks,)), dma((blocks,)),
            dma((blocks, pieces)), dma((blocks, pieces)),
            dma((blocks, pieces)), dma((blocks, pieces)),
        ],
        compiler_params=pltpu.CompilerParams(
            collective_id=0, has_side_effects=True, vmem_limit_bytes=56 * 2**20
        ),
        name="rebalanced_attention",
    )(block_live, left_count, right_count, node_tiles, kv_keys, kv_values, queries, hidden, out_weight)


def solution(mesh):
    return jax.shard_map(
        functools.partial(on_device, ring=mesh.shape["blk"]),
        mesh=mesh,
        in_specs=(
            P("blk", None, "tp"),
            P("blk", None, "tp"),
            P("blk", None, "tp"),
            P("blk", None, "tp"),
            P("tp", None),
            P("blk"),
            P("blk", None),
            P("blk"),
            P("blk"),
        ),
        out_specs=P("blk", None, "tp"),
        check_vma=False,
    )
```

```python
import functools
import math

import jax
import jax.numpy as jnp
from jax import lax
from jax.experimental import pallas as pl
from jax.experimental.pallas import tpu as pltpu
from jax.sharding import PartitionSpec as P

TILE = 128
HEAD = 128
S_MAX = 2
MASKED = -(2.0**100)
MESH = pl.DeviceIdType.MESH
ORDER = (0, 3, 1, 2)
GROUPS = ((0, 2), (2, 4), (4, 7))
PIECES = ((0, 256), (256, 512), (512, 896))
LAST_PIECES = ((0, 256), (256, 512), (512, 768), (768, 896))
CHUNK = 512


def pieces_of(j):
    return LAST_PIECES if j == ORDER[-1] else PIECES


def block_kernel(
    live_hbm, left_hbm, right_hbm, tiles_hbm, k_hbm, v_hbm, q_hbm, hid_hbm, w_hbm,
    out_ref,
    live_ref, left_ref, right_ref, tiles_ref,
    kb, vb, qb, hb, wb, ind, vt, far, sc, ab, keep, snd, rcv, cut,
    s_sem, k_sem, v_sem, q_sem, h_sem, w_sem, ws_sem, wr_sem, as_sem, ar_sem,
    is_sem, ir_sem, cs_sem, cr_sem,
    *, ring,
):
    blocks, tokens, _ = kb.shape
    nodes, width = qb.shape[1:]
    b = lax.axis_index("blk")
    t = lax.axis_index("tp")
    half = t // 2
    core = t % 2
    prev = (b + ring - 1) % ring
    following = (b + 1) % ring
    partner = (b, 2 * half + 1 - core)
    across = 2 * (1 - half) + core
    peer = (b, across)

    barrier = pltpu.get_barrier_semaphore()
    for other in (partner, peer, (prev, across), (following, across)):
        pl.semaphore_signal(barrier, inc=1, device_id=other, device_id_type=MESH)

    def local(src, dst, sem):
        return pltpu.make_async_copy(src, dst, sem)

    def remote(src, dst, send, recv, device):
        return pltpu.make_async_remote_copy(
            src_ref=src, dst_ref=dst, send_sem=send, recv_sem=recv,
            device_id=device, device_id_type=MESH,
        )

    q_copies = [local(q_hbm.at[j], qb.at[j], q_sem.at[j]) for j in range(blocks)]
    k_copies = [local(k_hbm.at[j], kb.at[j], k_sem.at[j]) for j in range(blocks)]
    v_copies = [local(v_hbm.at[j], vb.at[j], v_sem.at[j]) for j in range(blocks)]
    small = [
        local(tiles_hbm, tiles_ref, s_sem.at[0]),
        local(live_hbm, live_ref, s_sem.at[1]),
        local(left_hbm, left_ref, s_sem.at[2]),
        local(right_hbm, right_ref, s_sem.at[3]),
    ]
    hid_copy = local(hid_hbm, hb, h_sem)

    weight_parts = [(half, lo, hi) for lo, hi in PIECES] + [(1 - half, 0, width)]

    def weight_from(quarter, lo, hi):
        return w_hbm.at[:, pl.ds(pl.multiple_of(quarter * width + lo, HEAD), hi - lo)]

    near_w = [
        local(
            weight_from(2 * h + core, lo, hi),
            wb.at[h, pl.ds(0, width), pl.ds(lo, hi - lo)], w_sem.at[n],
        )
        for n, (h, lo, hi) in enumerate(weight_parts)
    ]
    far_w = [
        remote(
            weight_from(2 * h + 1 - core, lo, hi),
            wb.at[h, pl.ds(width, width), pl.ds(lo, hi - lo)],
            ws_sem.at[n], wr_sem.at[n], partner,
        )
        for n, (h, lo, hi) in enumerate(weight_parts)
    ]

    for copy in small[:1] + [q_copies[ORDER[0]], k_copies[ORDER[0]], v_copies[ORDER[0]]] + small[1:]:
        copy.start()
    for copy in near_w[:-1]:
        copy.start()
    q_copies[ORDER[1]].start()
    k_copies[ORDER[1]].start()
    v_copies[ORDER[1]].start()

    token = lax.broadcasted_iota(jnp.int32, (tokens, HEAD), 0)
    lane = lax.broadcasted_iota(jnp.int32, (tokens, HEAD), 1)
    ind[...] = jnp.where(token // TILE == lane, 1.0, 0.0).astype(jnp.bfloat16)
    vt[HEAD:, :] = jnp.ones((16, tokens), jnp.bfloat16)
    zero_rows = jnp.zeros((nodes, width), jnp.bfloat16)
    out_ref[S_MAX] = zero_rows
    out_ref[S_MAX + blocks - 1] = zero_rows
    small[0].wait()
    node_lane = lax.broadcasted_iota(jnp.int32, (nodes, HEAD), 1).astype(jnp.float32)
    for j in range(blocks):
        row = tiles_ref[pl.ds(j, 1), :].astype(jnp.float32)
        reach = jnp.transpose(jnp.broadcast_to(row, (HEAD, nodes)))
        far[j] = jnp.where(node_lane < reach, 0.0, MASKED).astype(jnp.bfloat16)

    def enter():
        pl.semaphore_wait(barrier, 4)
        for copy in far_w[:-1]:
            copy.start()

    scale = jnp.float32(HEAD**-0.5 * math.log2(math.e))
    swaps = ((0, GROUPS[1][1] * HEAD), (GROUPS[1][1] * HEAD, width))
    attn_copies = {
        (j, n): remote(
            ab.at[j, :, pl.ds(lo, hi - lo)], ab.at[j, :, pl.ds(width + lo, hi - lo)],
            as_sem.at[j, n], ar_sem.at[j, n], partner,
        )
        for j in range(blocks)
        for n, (lo, hi) in enumerate(swaps)
    }
    inner = {
        (j, n): remote(
            snd.at[j, :, pl.ds(lo, hi - lo)], rcv.at[j, :, pl.ds(lo, hi - lo)],
            is_sem.at[j, n], ir_sem.at[j, n], peer,
        )
        for j in range(blocks)
        for n, (lo, hi) in enumerate(pieces_of(j))
    }
    outer = {
        (j, n): remote(
            cut.at[j, :, pl.ds(lo, hi - lo)],
            out_ref.at[j + S_MAX + blocks if j < S_MAX else j - S_MAX, :, pl.ds(lo, hi - lo)],
            cs_sem.at[j, n], cr_sem.at[j, n],
            (prev if j < S_MAX else following, across),
        )
        for j in range(blocks)
        for n, (lo, hi) in enumerate(pieces_of(j))
    }

    def moved(j):
        if j == 1:
            return (left_ref[0] >= 2).astype(jnp.int32)
        if j == 2:
            return (right_ref[0] >= 2).astype(jnp.int32)
        return None

    def scores(j, g, slot):
        lo, hi = GROUPS[g]
        rows = (hi - lo) * nodes
        if g == 0:
            q_copies[j].wait()
            k_copies[j].wait()
        q_rows = jnp.concatenate(
            [qb[j, :, h * HEAD : (h + 1) * HEAD] for h in range(lo, hi)], axis=0
        )
        far_rows = jnp.concatenate([far[j]] * (hi - lo), axis=0)
        rhs = jnp.concatenate([q_rows, far_rows], axis=1)
        top = jnp.full((8, rows), -jnp.inf, jnp.float32)
        for c in range(0, tokens, CHUNK):
            lhs = jnp.concatenate([kb[j, c : c + CHUNK, :], ind[c : c + CHUNK, :]], axis=1)
            part = lax.dot_general(
                lhs, rhs, (((1,), (1,)), ((), ())), preferred_element_type=jnp.float32
            )
            sc[slot, c : c + CHUNK, :rows] = part
            top = jnp.maximum(top, jnp.max(part.reshape(CHUNK // 8, 8, rows), axis=0))
        return jnp.max(top, axis=0, keepdims=True)

    def mix(j, g, slot, top):
        lo, hi = GROUPS[g]
        rows = (hi - lo) * nodes
        if g == 0:
            v_copies[j].wait()
            for c in range(0, tokens, HEAD):
                vt[: HEAD, c : c + HEAD] = jnp.transpose(vb[j, c : c + HEAD, :])
        total = None
        for c in range(0, tokens, CHUNK):
            part = jnp.exp2((sc[slot, c : c + CHUNK, :rows] - top) * scale).astype(jnp.bfloat16)
            term = jnp.dot(vt[:, c : c + CHUNK], part, preferred_element_type=jnp.float32)
            total = term if total is None else total + term
        mean = total[:HEAD] / total[HEAD : HEAD + 1]
        for n, h in enumerate(range(lo, hi)):
            ab[j, :, h * HEAD : (h + 1) * HEAD] = jnp.transpose(
                mean[:, n * nodes : (n + 1) * nodes]
            ).astype(jnp.bfloat16)

    def residual(j, lo, hi, flag):
        rows = hb[j, :, lo:hi].astype(jnp.float32)
        return rows if flag is None else jnp.where(flag, rows, 0.0)

    def send_part(n):
        j = ORDER[n]
        for n_swap in range(len(swaps)):
            attn_copies[j, n_swap].wait()
        move = moved(j)
        pick = half if move is None else half * move + (1 - half) * (1 - move)
        sums = []
        for p, (lo, hi) in enumerate(pieces_of(j)):
            if n == 0:
                near_w[p].wait()
                far_w[p].wait()
            sums.append(jnp.dot(ab[j], wb[pick, :, lo:hi], preferred_element_type=jnp.float32))
            if n == 0 and p == 0:
                hid_copy.wait()
            if n == 0:
                hand_over(j, p, sums[p], move)
            elif p > 0:
                hand_over(j, p - 1, sums[p - 1], move)
        if n > 0:
            hand_over(j, len(sums) - 1, sums[-1], move)

    def hand_over(j, p, part, move):
        lo, hi = pieces_of(j)[p]
        part = part + residual(j, lo, hi, None if move is None else move == 1)
        snd[j, :, lo:hi] = part.astype(jnp.bfloat16)
        inner[j, p].start()

    def keep_part(n):
        j = ORDER[n]
        move = moved(j)
        if n == 0:
            near_w[-1].wait()
            far_w[-1].wait()
        pick = 1 - half if move is None else half * (1 - move) + (1 - half) * move
        for lo, hi in pieces_of(j):
            part = jnp.dot(ab[j], wb[pick, :, lo:hi], preferred_element_type=jnp.float32)
            if move is not None:
                part = part + residual(j, lo, hi, move == 0)
            keep[j, :, lo:hi] = part

    def settle(n, p):
        j = ORDER[n]
        lo, hi = pieces_of(j)[p]
        move = moved(j)
        inner[j, p].wait_recv()
        total = keep[j, :, lo:hi] + rcv[j, :, lo:hi].astype(jnp.float32)
        node = lax.broadcasted_iota(jnp.int32, total.shape, 0)
        live = live_ref[j]
        leaving = live if move is None else live * move
        cut[j, :, lo:hi] = jnp.where(node < leaving, total, 0.0).astype(jnp.bfloat16)
        outer[j, p].start()
        if move is not None:
            out_ref[S_MAX + j, :, lo:hi] = jnp.where(
                node < live * (1 - move), total, 0.0
            ).astype(jnp.bfloat16)

    def pass_on(n, part):
        attn_copies[ORDER[n], part].start()
        if n == 0 and part == 1:
            far_w[-1].start()

    groups = len(GROUPS)
    units = [(j, g) for j in ORDER for g in range(groups)]
    plan = {
        1: [(pass_on, 0, 0)],
        2: [(pass_on, 0, 1)],
        3: [(send_part, 0)],
        4: [(pass_on, 1, 0)],
        5: [(pass_on, 1, 1), (keep_part, 0), (settle, 0, 0), (send_part, 1), (settle, 0, 1)],
        7: [(pass_on, 2, 0), (settle, 0, 2)],
        8: [(pass_on, 2, 1), (keep_part, 1), (settle, 1, 0), (settle, 1, 1), (send_part, 2)],
        9: [(settle, 1, 2)],
        10: [(pass_on, 3, 0)],
        11: [(pass_on, 3, 1), (keep_part, 2), (settle, 2, 0), (send_part, 3), (settle, 2, 1),
             (keep_part, 3), (settle, 2, 2)]
        + [(settle, 3, p) for p in range(len(LAST_PIECES))],
    }
    for copy in small[1:]:
        copy.wait()
    top = scores(*units[0], 0)
    hid_copy.start()
    near_w[-1].start()
    for j in ORDER[2:]:
        q_copies[j].start()
        k_copies[j].start()
        v_copies[j].start()
    for u, (j, g) in enumerate(units):
        ahead = scores(*units[u + 1], (u + 1) % 2) if u + 1 < len(units) else None
        if u == 0:
            enter()
        mix(j, g, u % 2, top)
        top = ahead
        for step, *rest in plan.get(u, ()):
            step(*rest)
    for j in range(blocks):
        for n in range(len(pieces_of(j))):
            inner[j, n].wait_send()
            outer[j, n].wait()


def on_device(kv_keys, kv_values, queries, hidden, out_weight, block_live, node_tiles, left_count, right_count, *, ring):
    blocks, tokens, _ = kv_keys.shape
    nodes, width = queries.shape[1:]
    hbm = pl.BlockSpec(memory_space=pltpu.MemorySpace.HBM)
    vmem = pl.BlockSpec(memory_space=pltpu.MemorySpace.VMEM)
    rows = max(hi - lo for lo, hi in GROUPS) * nodes
    bf16, f32 = jnp.bfloat16, jnp.float32
    dma = pltpu.SemaphoreType.DMA
    pieces = max(len(PIECES), len(LAST_PIECES))
    parts = len(PIECES) + 1
    return pl.pallas_call(
        functools.partial(block_kernel, ring=ring),
        out_shape=pltpu.VMEM((blocks + 2 * S_MAX, nodes, width), bf16),
        in_specs=[hbm] * 9,
        out_specs=vmem,
        scratch_shapes=[
            pltpu.SMEM(block_live.shape, jnp.int32),
            pltpu.SMEM(left_count.shape, jnp.int32),
            pltpu.SMEM(right_count.shape, jnp.int32),
            pltpu.VMEM(node_tiles.shape, jnp.int32),
            pltpu.VMEM((blocks, tokens, HEAD), bf16),
            pltpu.VMEM((blocks, tokens, HEAD), bf16),
            pltpu.VMEM((blocks, nodes, width), bf16),
            pltpu.VMEM((blocks, nodes, width), bf16),
            pltpu.VMEM((2, 2 * width, width), bf16),
            pltpu.VMEM((tokens, HEAD), bf16),
            pltpu.VMEM((HEAD + 16, tokens), bf16),
            pltpu.VMEM((blocks, nodes, HEAD), bf16),
            pltpu.VMEM((2, tokens, rows), f32),
            pltpu.VMEM((blocks, nodes, 2 * width), bf16),
            pltpu.VMEM((blocks, nodes, width), f32),
            pltpu.VMEM((blocks, nodes, width), bf16),
            pltpu.VMEM((blocks, nodes, width), bf16),
            pltpu.VMEM((blocks, nodes, width), bf16),
            dma((4,)), dma((blocks,)), dma((blocks,)), dma((blocks,)), dma, dma((parts,)),
            dma((parts,)), dma((parts,)), dma((blocks, 2)), dma((blocks, 2)),
            dma((blocks, pieces)), dma((blocks, pieces)),
            dma((blocks, pieces)), dma((blocks, pieces)),
        ],
        compiler_params=pltpu.CompilerParams(
            collective_id=0, has_side_effects=True, vmem_limit_bytes=56 * 2**20
        ),
        name="rebalanced_attention",
    )(block_live, left_count, right_count, node_tiles, kv_keys, kv_values, queries, hidden, out_weight)


def solution(mesh):
    return jax.shard_map(
        functools.partial(on_device, ring=mesh.shape["blk"]),
        mesh=mesh,
        in_specs=(
            P("blk", None, "tp"),
            P("blk", None, "tp"),
            P("blk", None, "tp"),
            P("blk", None, "tp"),
            P("tp", None),
            P("blk"),
            P("blk", None),
            P("blk"),
            P("blk"),
        ),
        out_specs=P("blk", None, "tp"),
        check_vma=False,
    )
```

```python
import functools
import math

import jax
import jax.numpy as jnp
from jax import lax
from jax.experimental import pallas as pl
from jax.experimental.pallas import tpu as pltpu
from jax.sharding import PartitionSpec as P

TILE = 128
HEAD = 128
S_MAX = 2
MASKED = -(2.0**100)
MESH = pl.DeviceIdType.MESH
ORDER = (0, 3, 1, 2)
GROUPS = ((0, 2), (2, 4), (4, 7))
PIECES = ((0, 256), (256, 512), (512, 896))
LAST_PIECES = ((0, 256), (256, 512), (512, 768), (768, 896))
CHUNK = 512


def pieces_of(j):
    return LAST_PIECES if j == ORDER[-1] else PIECES


def block_kernel(
    live_hbm, left_hbm, right_hbm, tiles_hbm, k_hbm, v_hbm, q_hbm, hid_hbm, w_hbm,
    out_ref,
    live_ref, left_ref, right_ref, tiles_ref,
    kb, vb, qb, hb, wb, ind, vt, far, sc, ab, keep, snd, rcv, cut,
    s_sem, k_sem, v_sem, q_sem, h_sem, w_sem, ws_sem, wr_sem, as_sem, ar_sem,
    is_sem, ir_sem, cs_sem, cr_sem,
    *, ring,
):
    blocks, tokens, _ = kb.shape
    nodes, width = qb.shape[1:]
    b = lax.axis_index("blk")
    t = lax.axis_index("tp")
    half = t // 2
    core = t % 2
    prev = (b + ring - 1) % ring
    following = (b + 1) % ring
    partner = (b, 2 * half + 1 - core)
    across = 2 * (1 - half) + core
    peer = (b, across)

    barrier = pltpu.get_barrier_semaphore()
    for other in (partner, peer, (prev, across), (following, across)):
        pl.semaphore_signal(barrier, inc=1, device_id=other, device_id_type=MESH)

    def local(src, dst, sem):
        return pltpu.make_async_copy(src, dst, sem)

    def remote(src, dst, send, recv, device):
        return pltpu.make_async_remote_copy(
            src_ref=src, dst_ref=dst, send_sem=send, recv_sem=recv,
            device_id=device, device_id_type=MESH,
        )

    q_copies = [local(q_hbm.at[j], qb.at[j], q_sem.at[j]) for j in range(blocks)]
    k_copies = [local(k_hbm.at[j], kb.at[j], k_sem.at[j]) for j in range(blocks)]
    v_copies = [local(v_hbm.at[j], vb.at[j], v_sem.at[j]) for j in range(blocks)]
    small = [
        local(tiles_hbm, tiles_ref, s_sem.at[0]),
        local(live_hbm, live_ref, s_sem.at[1]),
        local(left_hbm, left_ref, s_sem.at[2]),
        local(right_hbm, right_ref, s_sem.at[3]),
    ]
    hid_copy = local(hid_hbm, hb, h_sem)

    weight_parts = [(half, lo, hi) for lo, hi in PIECES] + [(1 - half, 0, width)]

    def weight_from(quarter, lo, hi):
        return w_hbm.at[:, pl.ds(pl.multiple_of(quarter * width + lo, HEAD), hi - lo)]

    near_w = [
        local(
            weight_from(2 * h + core, lo, hi),
            wb.at[h, pl.ds(0, width), pl.ds(lo, hi - lo)], w_sem.at[n],
        )
        for n, (h, lo, hi) in enumerate(weight_parts)
    ]
    far_w = [
        remote(
            weight_from(2 * h + 1 - core, lo, hi),
            wb.at[h, pl.ds(width, width), pl.ds(lo, hi - lo)],
            ws_sem.at[n], wr_sem.at[n], partner,
        )
        for n, (h, lo, hi) in enumerate(weight_parts)
    ]

    for copy in small[:1] + [q_copies[ORDER[0]], k_copies[ORDER[0]], v_copies[ORDER[0]]] + small[1:]:
        copy.start()
    for copy in near_w[:-1]:
        copy.start()
    q_copies[ORDER[1]].start()
    k_copies[ORDER[1]].start()
    v_copies[ORDER[1]].start()

    token = lax.broadcasted_iota(jnp.int32, (tokens, HEAD), 0)
    lane = lax.broadcasted_iota(jnp.int32, (tokens, HEAD), 1)
    ind[...] = jnp.where(token // TILE == lane, 1.0, 0.0).astype(jnp.bfloat16)
    vt[HEAD:, :] = jnp.ones((16, tokens), jnp.bfloat16)
    zero_rows = jnp.zeros((nodes, width), jnp.bfloat16)
    out_ref[S_MAX] = zero_rows
    out_ref[S_MAX + blocks - 1] = zero_rows
    small[0].wait()
    node_lane = lax.broadcasted_iota(jnp.int32, (nodes, HEAD), 1).astype(jnp.float32)
    for j in range(blocks):
        row = tiles_ref[pl.ds(j, 1), :].astype(jnp.float32)
        reach = jnp.transpose(jnp.broadcast_to(row, (HEAD, nodes)))
        far[j] = jnp.where(node_lane < reach, 0.0, MASKED).astype(jnp.bfloat16)

    def enter():
        pl.semaphore_wait(barrier, 4)
        for copy in far_w[:-1]:
            copy.start()

    scale = jnp.float32(HEAD**-0.5 * math.log2(math.e))
    swaps = ((0, GROUPS[1][1] * HEAD), (GROUPS[1][1] * HEAD, width))
    attn_copies = {
        (j, n): remote(
            ab.at[j, :, pl.ds(lo, hi - lo)], ab.at[j, :, pl.ds(width + lo, hi - lo)],
            as_sem.at[j, n], ar_sem.at[j, n], partner,
        )
        for j in range(blocks)
        for n, (lo, hi) in enumerate(swaps)
    }
    inner = {
        (j, n): remote(
            snd.at[j, :, pl.ds(lo, hi - lo)], rcv.at[j, :, pl.ds(lo, hi - lo)],
            is_sem.at[j, n], ir_sem.at[j, n], peer,
        )
        for j in range(blocks)
        for n, (lo, hi) in enumerate(pieces_of(j))
    }
    outer = {
        (j, n): remote(
            cut.at[j, :, pl.ds(lo, hi - lo)],
            out_ref.at[j + S_MAX + blocks if j < S_MAX else j - S_MAX, :, pl.ds(lo, hi - lo)],
            cs_sem.at[j, n], cr_sem.at[j, n],
            (prev if j < S_MAX else following, across),
        )
        for j in range(blocks)
        for n, (lo, hi) in enumerate(pieces_of(j))
    }

    def moved(j):
        if j == 1:
            return (left_ref[0] >= 2).astype(jnp.int32)
        if j == 2:
            return (right_ref[0] >= 2).astype(jnp.int32)
        return None

    def scores(j, g, slot):
        lo, hi = GROUPS[g]
        rows = (hi - lo) * nodes
        if g == 0:
            q_copies[j].wait()
            k_copies[j].wait()
        q_rows = jnp.concatenate(
            [qb[j, :, h * HEAD : (h + 1) * HEAD] for h in range(lo, hi)], axis=0
        )
        far_rows = jnp.concatenate([far[j]] * (hi - lo), axis=0)
        rhs = jnp.concatenate([q_rows, far_rows], axis=1)
        top = jnp.full((8, rows), -jnp.inf, jnp.float32)
        for c in range(0, tokens, CHUNK):
            lhs = jnp.concatenate([kb[j, c : c + CHUNK, :], ind[c : c + CHUNK, :]], axis=1)
            part = lax.dot_general(
                lhs, rhs, (((1,), (1,)), ((), ())), preferred_element_type=jnp.float32
            )
            sc[slot, c : c + CHUNK, :rows] = part
            top = jnp.maximum(top, jnp.max(part.reshape(CHUNK // 8, 8, rows), axis=0))
        return jnp.max(top, axis=0, keepdims=True)

    def mix(j, g, slot, top):
        lo, hi = GROUPS[g]
        rows = (hi - lo) * nodes
        if g == 0:
            v_copies[j].wait()
            for c in range(0, tokens, HEAD):
                vt[: HEAD, c : c + HEAD] = jnp.transpose(vb[j, c : c + HEAD, :])
        total = None
        for c in range(0, tokens, CHUNK):
            part = jnp.exp2((sc[slot, c : c + CHUNK, :rows] - top) * scale).astype(jnp.bfloat16)
            term = jnp.dot(vt[:, c : c + CHUNK], part, preferred_element_type=jnp.float32)
            total = term if total is None else total + term
        mean = total[:HEAD] / total[HEAD : HEAD + 1]
        for n, h in enumerate(range(lo, hi)):
            ab[j, :, h * HEAD : (h + 1) * HEAD] = jnp.transpose(
                mean[:, n * nodes : (n + 1) * nodes]
            ).astype(jnp.bfloat16)

    def residual(j, lo, hi, flag):
        rows = hb[j, :, lo:hi].astype(jnp.float32)
        return rows if flag is None else jnp.where(flag, rows, 0.0)

    def send_part(n):
        j = ORDER[n]
        for n_swap in range(len(swaps)):
            attn_copies[j, n_swap].wait()
        move = moved(j)
        pick = half if move is None else half * move + (1 - half) * (1 - move)
        sums = []
        for p, (lo, hi) in enumerate(pieces_of(j)):
            if n == 0:
                near_w[p].wait()
                far_w[p].wait()
            sums.append(jnp.dot(ab[j], wb[pick, :, lo:hi], preferred_element_type=jnp.float32))
            if n == 0 and p == 0:
                hid_copy.wait()
            if n == 0:
                hand_over(j, p, sums[p], move)
            elif p > 0:
                hand_over(j, p - 1, sums[p - 1], move)
        if n > 0:
            hand_over(j, len(sums) - 1, sums[-1], move)

    def hand_over(j, p, part, move):
        lo, hi = pieces_of(j)[p]
        part = part + residual(j, lo, hi, None if move is None else move == 1)
        snd[j, :, lo:hi] = part.astype(jnp.bfloat16)
        inner[j, p].start()

    def keep_part(n):
        j = ORDER[n]
        move = moved(j)
        if n == 0:
            near_w[-1].wait()
            far_w[-1].wait()
        pick = 1 - half if move is None else half * (1 - move) + (1 - half) * move
        for lo, hi in pieces_of(j):
            part = jnp.dot(ab[j], wb[pick, :, lo:hi], preferred_element_type=jnp.float32)
            if move is not None:
                part = part + residual(j, lo, hi, move == 0)
            keep[j, :, lo:hi] = part

    def settle(n, p):
        j = ORDER[n]
        lo, hi = pieces_of(j)[p]
        move = moved(j)
        inner[j, p].wait_recv()
        total = keep[j, :, lo:hi] + rcv[j, :, lo:hi].astype(jnp.float32)
        node = lax.broadcasted_iota(jnp.int32, total.shape, 0)
        live = live_ref[j]
        leaving = live if move is None else live * move
        cut[j, :, lo:hi] = jnp.where(node < leaving, total, 0.0).astype(jnp.bfloat16)
        outer[j, p].start()
        if move is not None:
            out_ref[S_MAX + j, :, lo:hi] = jnp.where(
                node < live * (1 - move), total, 0.0
            ).astype(jnp.bfloat16)

    def pass_on(n, part):
        attn_copies[ORDER[n], part].start()
        if n == 0 and part == 1:
            far_w[-1].start()

    groups = len(GROUPS)
    units = [(j, g) for j in ORDER for g in range(groups)]
    plan = {
        1: [(pass_on, 0, 0)],
        2: [(pass_on, 0, 1)],
        3: [(send_part, 0)],
        4: [(pass_on, 1, 0)],
        5: [(pass_on, 1, 1), (keep_part, 0), (settle, 0, 0), (send_part, 1), (settle, 0, 1)],
        7: [(pass_on, 2, 0), (settle, 0, 2)],
        8: [(pass_on, 2, 1), (keep_part, 1), (settle, 1, 0), (settle, 1, 1), (send_part, 2)],
        9: [(settle, 1, 2)],
        10: [(pass_on, 3, 0)],
        11: [(pass_on, 3, 1), (keep_part, 2), (settle, 2, 0), (send_part, 3), (settle, 2, 1),
             (keep_part, 3), (settle, 2, 2)]
        + [(settle, 3, p) for p in range(len(LAST_PIECES))],
    }
    for copy in small[1:]:
        copy.wait()
    top = scores(*units[0], 0)
    hid_copy.start()
    near_w[-1].start()
    for j in ORDER[2:]:
        q_copies[j].start()
        k_copies[j].start()
        v_copies[j].start()
    for u, (j, g) in enumerate(units):
        ahead = scores(*units[u + 1], (u + 1) % 2) if u + 1 < len(units) else None
        if u == 0:
            enter()
        mix(j, g, u % 2, top)
        top = ahead
        for step, *rest in plan.get(u, ()):
            with jax.named_scope(step.__name__):
                step(*rest)
    for j in range(blocks):
        for n in range(len(pieces_of(j))):
            inner[j, n].wait_send()
            outer[j, n].wait()


def on_device(kv_keys, kv_values, queries, hidden, out_weight, block_live, node_tiles, left_count, right_count, *, ring):
    blocks, tokens, _ = kv_keys.shape
    nodes, width = queries.shape[1:]
    hbm = pl.BlockSpec(memory_space=pltpu.MemorySpace.HBM)
    vmem = pl.BlockSpec(memory_space=pltpu.MemorySpace.VMEM)
    rows = max(hi - lo for lo, hi in GROUPS) * nodes
    bf16, f32 = jnp.bfloat16, jnp.float32
    dma = pltpu.SemaphoreType.DMA
    pieces = max(len(PIECES), len(LAST_PIECES))
    parts = len(PIECES) + 1
    return pl.pallas_call(
        functools.partial(block_kernel, ring=ring),
        out_shape=pltpu.VMEM((blocks + 2 * S_MAX, nodes, width), bf16),
        in_specs=[hbm] * 9,
        out_specs=vmem,
        scratch_shapes=[
            pltpu.SMEM(block_live.shape, jnp.int32),
            pltpu.SMEM(left_count.shape, jnp.int32),
            pltpu.SMEM(right_count.shape, jnp.int32),
            pltpu.VMEM(node_tiles.shape, jnp.int32),
            pltpu.VMEM((blocks, tokens, HEAD), bf16),
            pltpu.VMEM((blocks, tokens, HEAD), bf16),
            pltpu.VMEM((blocks, nodes, width), bf16),
            pltpu.VMEM((blocks, nodes, width), bf16),
            pltpu.VMEM((2, 2 * width, width), bf16),
            pltpu.VMEM((tokens, HEAD), bf16),
            pltpu.VMEM((HEAD + 16, tokens), bf16),
            pltpu.VMEM((blocks, nodes, HEAD), bf16),
            pltpu.VMEM((2, tokens, rows), f32),
            pltpu.VMEM((blocks, nodes, 2 * width), bf16),
            pltpu.VMEM((blocks, nodes, width), f32),
            pltpu.VMEM((blocks, nodes, width), bf16),
            pltpu.VMEM((blocks, nodes, width), bf16),
            pltpu.VMEM((blocks, nodes, width), bf16),
            dma((4,)), dma((blocks,)), dma((blocks,)), dma((blocks,)), dma, dma((parts,)),
            dma((parts,)), dma((parts,)), dma((blocks, 2)), dma((blocks, 2)),
            dma((blocks, pieces)), dma((blocks, pieces)),
            dma((blocks, pieces)), dma((blocks, pieces)),
        ],
        compiler_params=pltpu.CompilerParams(
            collective_id=0, has_side_effects=True, vmem_limit_bytes=56 * 2**20
        ),
        name="rebalanced_attention",
    )(block_live, left_count, right_count, node_tiles, kv_keys, kv_values, queries, hidden, out_weight)


def solution(mesh):
    return jax.shard_map(
        functools.partial(on_device, ring=mesh.shape["blk"]),
        mesh=mesh,
        in_specs=(
            P("blk", None, "tp"),
            P("blk", None, "tp"),
            P("blk", None, "tp"),
            P("blk", None, "tp"),
            P("tp", None),
            P("blk"),
            P("blk", None),
            P("blk"),
            P("blk"),
        ),
        out_specs=P("blk", None, "tp"),
        check_vma=False,
    )
```
